32 devices in a mesh: groups: 2 (over y), tensor: 4 (over z), dp: 2 (over x), kv: 2 (over core).
Axes of the slice: x: 2, y: 2, z: 4, core: 2. Of those that a mesh axis runs over, the one named last changes fastest.
Arguments:
- residual: bfloat16 [64, 16384], P(('groups', 'dp'), ('tensor', 'kv')), parts along dimension 0, may hold values from -10 to 10
- query: bfloat16 [64, 8192], P(('groups', 'dp'), ('tensor', 'kv')), parts along dimension 0, may hold values from -60 to 60
- new_pair: bfloat16 [2, 64, 4, 128], P(None, ('groups', 'dp')), parts along dimension 1, may hold values from -8 to 8
- kv_cache: bfloat16 [2, 64, 2048, 4, 128], P(None, ('groups', 'dp'), ('tensor', 'kv')), parts along dimension 1, may hold values from -4.5 to 4.5
- lengths: int32 [64], P(('groups', 'dp')), parts along dimension 0, may hold values from 2 to 2048
- out_weight: bfloat16 [8192, 16384], P(('tensor', 'kv')), may hold values from -0.09375 to 0.09375
- norm_gain: bfloat16 [16384], replicated, may hold values from 0.25 to 1.75
Outputs:
- residual_out: bfloat16 [64, 16384], P(('groups', 'dp'), ('tensor', 'kv')), parts along dimension 0
- mlp_input: bfloat16 [64, 16384], P(('groups', 'dp')), parts along dimension 0
The draws below stay inside these ranges and needn't reach their ends.
There are 2 independent parts, one for each index of `groups`. The reference program is written for one: setup_inputs(seed, part) draws one part's arguments, and reference() takes and returns one part's arrays. A program takes and returns all parts, laid end to end along the dimension named above; an argument that names none is the same for every part. Nothing has to cross between parts.
Inputs may be any that keep to these rules, and one draw needn't show every extreme that they name: Positions below lengths[b] hold sequence b's cache; the others are ignored.
All inputs are finite; a program needn't handle non-finite values.
Results may differ from the reference program's by a relative error of at most 0.007.
Values may be sent and summed in bfloat16 or wider, within the bound.
No kernel may reach another device: no remote copies, remote signals or barrier semaphores. Data moves between devices by JAX's collectives and lax.ppermute only.
A program may use at most 128 MiB of HBM per device.

```python
import math
import jax
import jax.numpy as jnp
from jax import lax

D = 16384
QH = 64
KVH = 4
HD = 128
MAXLEN = 2048
B = 32


def cache_values(key):
    shape = (2, B, MAXLEN, KVH, HD)
    base = jnp.clip(jax.random.normal(jax.random.fold_in(key, 101), shape, jnp.float32), -4.5, 4.5)
    return base


def draw_kv_cache(key, part):
    return cache_values(key).astype(jnp.bfloat16)


def draw_query(key, part):
    drawn = jnp.clip(1.5 * jax.random.normal(jax.random.fold_in(key, 202), (B, QH, HD), jnp.float32), -9.0, 9.0)
    return drawn.reshape(B, QH * HD).astype(jnp.bfloat16)


def draw_residual(key, part):
    noise_key = jax.random.fold_in(key, 303)
    column_key = jax.random.fold_in(key, 304)
    row_key = jax.random.fold_in(key, 305)
    columns = jnp.arange(D, dtype=jnp.float32) / D
    column_scale = jnp.exp(jax.random.uniform(column_key, (D,), jnp.float32, 0.0, math.log(10.0)))
    row_scale = jnp.exp(jax.random.uniform(row_key, (B, 1), jnp.float32, 0.0, math.log(10.0)))
    raw = jnp.clip(jax.random.normal(noise_key, (B, D), jnp.float32), -6.0, 6.0)
    rising = jnp.power(3.0, columns)
    base = 0.005
    return (base * raw * rising[None, :] * column_scale[None, :] * row_scale).astype(jnp.bfloat16)


def set_ends(drawn, rng, low, largest):
    longest = drawn.shape.index(max(drawn.shape))
    spots = []
    for shift in (0, 1):
        where = [jax.random.randint(jax.random.fold_in(rng, axis), (), 0, length) for axis, length in enumerate(drawn.shape)]
        where[longest] = (where[longest] + shift) % drawn.shape[longest]
        spots.append(tuple(where))
    return drawn.at[spots[0]].set(low).at[spots[1]].set(largest)


def spiked(array, stream_key, source, target, shards_of, factor):
    def block_of(dim):
        return (jnp.arange(array.shape[dim]) // (array.shape[dim] // shards_of)).reshape((-1,) + (1,) * (array.ndim - 1 - dim))

    one_side = jax.random.permutation(stream_key, shards_of)[block_of(target)]
    other_side = (block_of(target) + shards_of // 2) % shards_of
    return jnp.where((block_of(source) == one_side) | (block_of(source) == other_side), factor * array, array)


def levels(rng, shape, split, smallest, top_value):
    gain, own = 1.0, jax.random.fold_in(rng, 6)
    for dim, parts in split:
        steps = jnp.exp(jax.random.uniform(jax.random.fold_in(own, dim), (parts,), jnp.float32, smallest / len(split), top_value / len(split)))
        gain = gain * jnp.repeat(steps, shape[dim] // parts).reshape([-1 if axis == dim else 1 for axis in range(len(shape))])
    return gain


def bell_draw(rng, dims, spread, limit, shards=(), kind=jnp.bfloat16):
    array = spread * jax.random.normal(rng, dims, jnp.float32)
    if shards:
        array = array * levels(rng, dims, shards, -0.22, 0.18)
    return jnp.clip(array, -limit, limit).astype(kind)


def noise_with(key, shape, deviation, most, cuts, heavy, kind=jnp.bfloat16):
    drawn = deviation * jax.random.normal(key, shape, jnp.float32)
    if cuts:
        drawn = drawn * levels(key, shape, cuts, -0.22, 0.18)
    return jnp.clip(spiked(drawn, jax.random.fold_in(key, 3), *heavy), -most, most).astype(kind)


def setup_inputs(seed: int = 0, part: int = 0) -> dict:
    splits = jax.random.split(jax.random.key(seed), 8)
    part_splits = jax.random.split(jax.random.fold_in(splits[7], part), 8)
    return {
        "residual": draw_residual(jax.random.fold_in(jax.random.fold_in(splits[7], part), 71), part),
        "query": draw_query(jax.random.fold_in(jax.random.fold_in(splits[7], part), 71), part),
        "new_pair": bell_draw(part_splits[2], (2, B, KVH, HD), 1.5, 8.0, ((1, 2),)),
        "kv_cache": draw_kv_cache(jax.random.fold_in(jax.random.fold_in(splits[7], part), 71), part),
        "lengths": set_ends(jax.random.randint(part_splits[4], (B,), 2, MAXLEN + 1), jax.random.fold_in(part_splits[4], 1), 2, MAXLEN).astype(jnp.int32),
        "out_weight": noise_with(splits[5], (QH * HD, D), (QH * HD) ** -0.5, 0.09375, ((0, 8),), (0, 1, 8, 2.0)),
        "norm_gain": jnp.clip(1.0 + 0.15 * jax.random.normal(splits[6], (D,), jnp.float32), 0.25, 1.75).astype(jnp.bfloat16),
    }


floor_value = -1e+30
epsilon = 1e-05

def reference(residual, query, new_pair, kv_cache, lengths, out_weight, norm_gain):
    batch = residual.shape[0]
    group = QH // KVH
    scaling = 1.0 / math.sqrt(HD)
    grouped = query.astype(jnp.float32).reshape(batch, KVH, group, HD)
    keys = kv_cache[0].astype(jnp.float32)
    values = kv_cache[1].astype(jnp.float32)
    scores = jnp.einsum('bgjd,bpgd->bgjp', grouped, keys, precision=lax.Precision.HIGHEST) * scaling
    places = jnp.arange(MAXLEN, dtype=jnp.int32)
    live = (places[None, :] < lengths[:, None])[:, None, None, :]
    scores = jnp.where(live, scores, floor_value)
    fresh_key = new_pair[0].astype(jnp.float32)
    fresh_value = new_pair[1].astype(jnp.float32)
    fresh = jnp.einsum('bgjd,bgd->bgj', grouped, fresh_key, precision=lax.Precision.HIGHEST) * scaling
    highest = jnp.maximum(lax.optimization_barrier(jnp.max(scores, axis=3)), fresh)
    weights = jnp.where(live, jnp.exp(scores - highest[..., None]), 0.0)
    fresh_weight = jnp.exp(fresh - highest)
    totals = lax.optimization_barrier(jnp.sum(weights, axis=3)) + fresh_weight
    accum = jnp.einsum('bgjp,bpgd->bgjd', weights, values, precision=lax.Precision.HIGHEST)
    accum = accum + fresh_weight[..., None] * fresh_value[:, :, None, :]
    attended = (accum / totals[..., None]).astype(jnp.bfloat16).reshape(batch, QH * HD)
    projected = jnp.dot(attended, out_weight, preferred_element_type=jnp.float32)
    stream = (residual.astype(jnp.float32) + projected).astype(jnp.bfloat16)
    widened = stream.astype(jnp.float32)
    mean_square = lax.optimization_barrier(jnp.mean(widened * widened, axis=1))
    normed = widened * lax.rsqrt(mean_square + epsilon)[:, None] * norm_gain.astype(jnp.float32)[None, :]
    return (stream, normed.astype(jnp.bfloat16))
```

```python
import functools
import math

import jax
import jax.numpy as jnp
from jax import lax
from jax.experimental import pallas as pl
from jax.experimental.pallas import tpu as pltpu
from jax.sharding import PartitionSpec as P

HD = 128
floor_value = -1e30
epsilon = 1e-05
F32 = jnp.float32
BF16 = jnp.bfloat16


def cost(flops, nbytes):
    return pl.CostEstimate(flops=flops, bytes_accessed=nbytes, transcendentals=0)


def diagonal(rows):
    return lax.broadcasted_iota(jnp.int32, (rows, HD), 0) == lax.broadcasted_iota(
        jnp.int32, (rows, HD), 1
    )


def to_row(column, eye):
    return jnp.sum(jnp.where(eye, column, 0.0), axis=0, keepdims=True)


def to_column(row, eye):
    return jnp.sum(jnp.where(eye, jnp.broadcast_to(row, eye.shape), 0.0), axis=1, keepdims=True)


def attention_kernel(
    chips, per_dev, kvh, group, step_seqs, where_ref, len_ref, q_ref, kv_ref, own_ref, par_ref, lse_ref
):
    step = pl.program_id(0)
    t, k, start = where_ref[0], where_ref[1], where_ref[2]
    heads, wide = q_ref.shape[1], kv_ref.shape[2]
    half = heads // 2
    scaling = 1.0 / math.sqrt(HD)
    row = lax.broadcasted_iota(jnp.int32, (heads, 1), 0)
    kk = row // half
    s = (row % half) // per_dev
    chip = (t - s + chips) % chips
    side = jnp.where(kk == 0, k, 1 - k)
    row_group = ((chip * 2 + side) * per_dev + row % per_dev) // group
    col = lax.broadcasted_iota(jnp.int32, (heads, wide), 1)
    same = (col % kvh) == row_group
    for i in range(step_seqs):
        b = step * step_seqs + i
        valid = same & (col < (len_ref[b] - start) * kvh)
        scores = (
            lax.dot_general(
                q_ref[i], kv_ref[0, i], (((1,), (1,)), ((), ())), preferred_element_type=F32
            )
            * scaling
        )
        scores = jnp.where(valid, scores, floor_value)
        top = jnp.max(scores, axis=1, keepdims=True)
        weights = jnp.where(valid, jnp.exp(scores - top), 0.0)
        total = jnp.sum(weights, axis=1, keepdims=True)
        acc = jnp.dot(weights.astype(BF16), kv_ref[1, i], preferred_element_type=F32)
        some = total > 0.0
        safe = jnp.where(some, total, 1.0)
        out = acc / safe
        lse = jnp.where(some, top + jnp.log(safe), floor_value)
        lse = jnp.broadcast_to(lse, (heads, HD))
        for side_index, ref in ((0, own_ref), (1, par_ref)):
            for piece in range(chips):
                first = side_index * half + piece * per_dev
                ref[piece, b] = out[first : first + per_dev]
                lse_ref[side_index, piece, b] = lse[first : first + per_dev]

    @pl.when(step == pl.num_programs(0) - 1)
    def _():
        seqs = own_ref.shape[1]
        eye = diagonal(seqs * per_dev)
        for side_index, ref in ((0, own_ref), (1, par_ref)):
            ref[chips] = jnp.zeros(ref.shape[1:], F32)
            for piece in range(chips):
                column = lse_ref[side_index, piece].reshape(seqs * per_dev, HD)
                ref[chips, piece // per_dev, piece % per_dev : piece % per_dev + 1, :] = to_row(
                    column, eye
                )


def pair_kernel(chips, per_dev, own_ref, par_ref, keep_ref, *send_refs):
    seqs = own_ref.shape[1]
    rows = seqs * per_dev
    eye = diagonal(rows)
    for piece in range(chips):
        at = (chips, piece // per_dev, slice(piece % per_dev, piece % per_dev + 1))
        first, second = to_column(own_ref[at], eye), to_column(par_ref[at], eye)
        top = jnp.maximum(first, second)
        w1, w2 = jnp.exp(first - top), jnp.exp(second - top)
        total = w1 + w2
        merged = (
            own_ref[piece].reshape(rows, HD) * w1 + par_ref[piece].reshape(rows, HD) * w2
        ) / total
        lse = to_row(top + jnp.log(total), eye)
        if piece == 0:
            keep_ref[:rows] = merged
            keep_ref[rows:] = jnp.broadcast_to(lse, (8, HD))
        else:
            out = send_refs[piece - 1]
            high = lse.astype(BF16).astype(F32)
            middle = (lse - high).astype(BF16).astype(F32)
            low = lse - high - middle
            out[:rows] = merged.astype(BF16)
            which = lax.broadcasted_iota(jnp.int32, (16, HD), 0)
            out[rows:] = jnp.where(
                which == 0, high, jnp.where(which == 1, middle, jnp.where(which == 2, low, 0.0))
            ).astype(BF16)


def owner_kernel(chips, per_dev, q_ref, k_ref, v_ref, keep_ref, *refs):
    arrived, out_ref, hold_ref = refs[: chips - 1], refs[chips - 1], refs[chips]
    rows = q_ref.shape[0]
    seqs = rows // per_dev
    eye = diagonal(rows)
    fresh = jnp.sum(
        q_ref[...].astype(F32) * k_ref[...].astype(F32), axis=1, keepdims=True
    ) * (1.0 / math.sqrt(HD))
    lses = [fresh, to_column(keep_ref[rows : rows + 1], eye)]
    for ref in arrived:
        extra = ref[rows:].astype(F32)
        lses.append(to_column(extra[0:1] + extra[1:2] + extra[2:3], eye))
    top = functools.reduce(jnp.maximum, lses)
    factors = [jnp.exp(lse - top) for lse in lses]
    total = functools.reduce(jnp.add, factors)
    acc = v_ref[...].astype(F32) * factors[0] + keep_ref[:rows] * factors[1]
    for ref, factor in zip(arrived, factors[2:]):
        acc = acc + ref[:rows].astype(F32) * factor
    hold_ref[...] = acc / total
    for j in range(per_dev):
        out_ref[:, j * HD : (j + 1) * HD] = hold_ref[pl.ds(j, seqs, stride=per_dev), :].astype(BF16)


def project_kernel(where_ref, x_ref, w_ref, o_ref):
    o_ref[0] = jnp.dot(x_ref[...], w_ref[...], preferred_element_type=F32)


def norm_kernel(chips, full, where_ref, gain_ref, *refs):
    pieces, out_ref = refs[: 2 * chips], refs[2 * chips]
    t, k = where_ref[0], where_ref[1]
    width = pieces[0].shape[1]
    total = jnp.zeros((pieces[0].shape[0], HD), F32)
    for ref in pieces:
        for c in range(0, width, HD):
            wide = ref[:, c : c + HD].astype(F32)
            total = total + wide * wide
    inverse = lax.rsqrt(jnp.sum(total, axis=1, keepdims=True) / full + epsilon)
    for index, ref in enumerate(pieces):
        side, s = index // chips, index % chips
        place = ((t - s + chips) % chips) * 2 + (k if side == 0 else 1 - k)
        at = pl.ds(pl.multiple_of(place * width, width), width)
        out_ref[:, at] = (ref[...].astype(F32) * inverse * gain_ref[:, at]).astype(BF16)


def on_device(chips, residual, query, new_pair, kv_cache, lengths, out_weight, norm_gain):
    seqs, width = residual.shape
    per_dev = query.shape[1] // HD
    span, kvh = kv_cache.shape[2], kv_cache.shape[3]
    heads = 2 * chips * per_dev
    group = heads // kvh
    rows = seqs * per_dev
    t, k = lax.axis_index("tensor"), lax.axis_index("kv")
    mine = t * 2 + k
    where = jnp.stack([t, k, mine * span]).astype(jnp.int32)

    def hop(x, s):
        return lax.ppermute(x, "tensor", [(i, (i + s) % chips) for i in range(chips)])

    def swap(x):
        return lax.ppermute(x, "kv", [(0, 1), (1, 0)])

    def everywhere(x):
        own = [x] + [hop(x, s) for s in range(1, chips)]
        return own + [swap(piece) for piece in own]

    vmem = pl.BlockSpec(memory_space=pltpu.VMEM)
    smem = pl.BlockSpec(memory_space=pltpu.SMEM)

    own_query = query.reshape(seqs, per_dev, HD)
    queries = jnp.concatenate(everywhere(own_query), axis=1)
    cache = kv_cache.reshape(2, seqs, span * kvh, HD)

    step_seqs = 2
    packed = jax.ShapeDtypeStruct((chips + 1, seqs, per_dev, HD), F32)
    whole_block = pl.BlockSpec((chips + 1, seqs, per_dev, HD), lambda i: (0, 0, 0, 0))
    own, par = pl.pallas_call(
        functools.partial(attention_kernel, chips, per_dev, kvh, group, step_seqs),
        grid=(seqs // step_seqs,),
        in_specs=[
            smem,
            smem,
            pl.BlockSpec((step_seqs, heads, HD), lambda i: (i, 0, 0)),
            pl.BlockSpec((2, step_seqs, span * kvh, HD), lambda i: (0, i, 0, 0)),
        ],
        out_specs=[whole_block, whole_block],
        out_shape=[packed, packed],
        scratch_shapes=[pltpu.VMEM((2, chips, seqs, per_dev, HD), F32)],
        compiler_params=pltpu.CompilerParams(
            dimension_semantics=("arbitrary",), vmem_limit_bytes=16 << 20
        ),
        cost_estimate=cost(4 * seqs * heads * span * kvh * HD, cache.size * 2),
        name="attention",
    )(where, lengths, queries, cache)

    sent = swap(par)
    merged = pl.pallas_call(
        functools.partial(pair_kernel, chips, per_dev),
        in_specs=[vmem, vmem],
        out_specs=[vmem] * chips,
        out_shape=[jax.ShapeDtypeStruct((rows + 8, HD), F32)]
        + [jax.ShapeDtypeStruct((rows + 16, HD), BF16)] * (chips - 1),
        compiler_params=pltpu.CompilerParams(vmem_limit_bytes=8 << 20),
        name="pair_merge",
    )(own, sent)
    arrived = [hop(merged[s], chips - s) for s in range(1, chips)]

    fresh_pair = lax.dynamic_index_in_dim(new_pair, mine * per_dev // group, 2, keepdims=False)
    fresh_pair = jnp.broadcast_to(fresh_pair[:, :, None, :], (2, seqs, per_dev, HD)).reshape(2, rows, HD)
    attended = pl.pallas_call(
        functools.partial(owner_kernel, chips, per_dev),
        in_specs=[vmem] * (chips + 3),
        out_specs=vmem,
        out_shape=jax.ShapeDtypeStruct((seqs, per_dev * HD), BF16),
        scratch_shapes=[pltpu.VMEM((rows, HD), F32)],
        compiler_params=pltpu.CompilerParams(vmem_limit_bytes=8 << 20),
        name="owner_merge",
    )(own_query.reshape(rows, HD), fresh_pair[0], fresh_pair[1], merged[0], *arrived)

    depth = out_weight.shape[0]
    tile = min(width, 1024)
    cut = width // tile

    def project(other):
        def column(s, c, at):
            side = 1 - at[1] if other else at[1]
            return (0, (((at[0] - s + chips) % chips) * 2 + side) * cut + c)

        return pl.pallas_call(
            project_kernel,
            grid_spec=pltpu.PrefetchScalarGridSpec(
                num_scalar_prefetch=1,
                grid=(chips, cut),
                in_specs=[
                    pl.BlockSpec((seqs, depth), lambda s, c, at: (0, 0)),
                    pl.BlockSpec((depth, tile), column),
                ],
                out_specs=pl.BlockSpec((1, seqs, tile), lambda s, c, at: (s, 0, c)),
            ),
            out_shape=jax.ShapeDtypeStruct((chips, seqs, width), F32),
            compiler_params=pltpu.CompilerParams(
                dimension_semantics=("arbitrary", "arbitrary"), vmem_limit_bytes=16 << 20
            ),
            cost_estimate=cost(
                2 * seqs * depth * width * chips, depth * width * chips * 2
            ),
            name="project_other" if other else "project_own",
        )(where, attended, out_weight)

    theirs = swap(project(True))
    ours = project(False)
    share = residual.astype(F32) + (ours[0] + theirs[0])
    for s in range(1, chips):
        share = share + hop((ours[s] + theirs[s]).astype(BF16), chips - s).astype(F32)
    stream = share.astype(BF16)

    pieces = everywhere(stream)
    normed = pl.pallas_call(
        functools.partial(norm_kernel, chips, width * chips * 2),
        in_specs=[smem] + [vmem] * (1 + 2 * chips),
        out_specs=vmem,
        out_shape=jax.ShapeDtypeStruct((seqs, width * chips * 2), BF16),
        compiler_params=pltpu.CompilerParams(vmem_limit_bytes=8 << 20),
        name="norm",
    )(where, norm_gain.astype(F32)[None, :], *pieces)
    return (stream, normed)


def solution(mesh):
    placed = (
        P(("groups", "dp"), ("tensor", "kv")),
        P(("groups", "dp"), ("tensor", "kv")),
        P(None, ("groups", "dp"), None, None),
        P(None, ("groups", "dp"), ("tensor", "kv"), None, None),
        P(("groups", "dp")),
        P(("tensor", "kv"), None),
        P(),
    )
    return jax.shard_map(
        functools.partial(on_device, mesh.shape["tensor"]),
        mesh=mesh,
        in_specs=placed,
        out_specs=(P(("groups", "dp"), ("tensor", "kv")), P(("groups", "dp"), None)),
        check_vma=False,
    )
```

```python
import functools
import math

import jax
import jax.numpy as jnp
from jax import lax
from jax.experimental import pallas as pl
from jax.experimental.pallas import tpu as pltpu
from jax.sharding import PartitionSpec as P

HD = 128
floor_value = -1e30
epsilon = 1e-05
F32 = jnp.float32
BF16 = jnp.bfloat16


def cost(flops, nbytes):
    return pl.CostEstimate(flops=flops, bytes_accessed=nbytes, transcendentals=0)


def diagonal(rows):
    return lax.broadcasted_iota(jnp.int32, (rows, HD), 0) == lax.broadcasted_iota(
        jnp.int32, (rows, HD), 1
    )


def to_row(column, eye):
    return jnp.sum(jnp.where(eye, column, 0.0), axis=0, keepdims=True)


def to_column(row, eye):
    return jnp.sum(jnp.where(eye, jnp.broadcast_to(row, eye.shape), 0.0), axis=1, keepdims=True)


def attention_kernel(
    chips, per_dev, kvh, group, step_seqs, where_ref, len_ref, q_ref, kv_ref, own_ref, par_ref, lse_ref
):
    step = pl.program_id(0)
    t, k, start = where_ref[0], where_ref[1], where_ref[2]
    heads, wide = q_ref.shape[1], kv_ref.shape[2]
    half = heads // 2
    scaling = 1.0 / math.sqrt(HD)
    row = lax.broadcasted_iota(jnp.int32, (heads, 1), 0)
    kk = row // half
    s = (row % half) // per_dev
    chip = (t - s + chips) % chips
    side = jnp.where(kk == 0, k, 1 - k)
    row_group = ((chip * 2 + side) * per_dev + row % per_dev) // group
    col = lax.broadcasted_iota(jnp.int32, (heads, wide), 1)
    col = jnp.where((col % kvh) == row_group, col, wide)
    for i in range(step_seqs):
        b = step * step_seqs + i
        valid = col < jnp.minimum((len_ref[b] - start) * kvh, wide)
        scores = (
            lax.dot_general(
                q_ref[i], kv_ref[0, i], (((1,), (1,)), ((), ())), preferred_element_type=F32
            )
            * scaling
        )
        scores = jnp.where(valid, scores, floor_value)
        top = jnp.max(scores, axis=1, keepdims=True)
        weights = jnp.exp(scores - top)
        total = jnp.sum(weights, axis=1, keepdims=True)
        acc = jnp.dot(weights.astype(BF16), kv_ref[1, i], preferred_element_type=F32)
        some = top > 0.5 * floor_value
        out = jnp.where(some, acc / total, 0.0)
        lse = jnp.where(some, top + jnp.log(total), floor_value)
        lse = jnp.broadcast_to(lse, (heads, HD))
        for side_index, ref in ((0, own_ref), (1, par_ref)):
            for piece in range(chips):
                first = side_index * half + piece * per_dev
                ref[piece, b] = out[first : first + per_dev]
                lse_ref[side_index, piece, b] = lse[first : first + per_dev]

    @pl.when(step == pl.num_programs(0) - 1)
    def _():
        seqs = own_ref.shape[1]
        eye = diagonal(seqs * per_dev)
        for side_index, ref in ((0, own_ref), (1, par_ref)):
            ref[chips] = jnp.zeros(ref.shape[1:], F32)
            for piece in range(chips):
                column = lse_ref[side_index, piece].reshape(seqs * per_dev, HD)
                ref[chips, piece // per_dev, piece % per_dev : piece % per_dev + 1, :] = to_row(
                    column, eye
                )


def pair_kernel(chips, per_dev, own_ref, par_ref, keep_ref, *send_refs):
    seqs = own_ref.shape[1]
    rows = seqs * per_dev
    eye = diagonal(rows)
    for piece in range(chips):
        at = (chips, piece // per_dev, slice(piece % per_dev, piece % per_dev + 1))
        first, second = to_column(own_ref[at], eye), to_column(par_ref[at], eye)
        top = jnp.maximum(first, second)
        w1, w2 = jnp.exp(first - top), jnp.exp(second - top)
        total = w1 + w2
        merged = (
            own_ref[piece].reshape(rows, HD) * w1 + par_ref[piece].reshape(rows, HD) * w2
        ) / total
        lse = to_row(top + jnp.log(total), eye)
        if piece == 0:
            keep_ref[:rows] = merged
            keep_ref[rows:] = jnp.broadcast_to(lse, (8, HD))
        else:
            out = send_refs[piece - 1]
            high = lse.astype(BF16).astype(F32)
            middle = (lse - high).astype(BF16).astype(F32)
            low = lse - high - middle
            out[:rows] = merged.astype(BF16)
            which = lax.broadcasted_iota(jnp.int32, (16, HD), 0)
            out[rows:] = jnp.where(
                which == 0, high, jnp.where(which == 1, middle, jnp.where(which == 2, low, 0.0))
            ).astype(BF16)


def owner_kernel(chips, per_dev, q_ref, k_ref, v_ref, keep_ref, *refs):
    arrived, out_ref, hold_ref = refs[: chips - 1], refs[chips - 1], refs[chips]
    rows = q_ref.shape[0]
    seqs = rows // per_dev
    eye = diagonal(rows)
    fresh = jnp.sum(
        q_ref[...].astype(F32) * k_ref[...].astype(F32), axis=1, keepdims=True
    ) * (1.0 / math.sqrt(HD))
    lses = [fresh, to_column(keep_ref[rows : rows + 1], eye)]
    for ref in arrived:
        extra = ref[rows:].astype(F32)
        lses.append(to_column(extra[0:1] + extra[1:2] + extra[2:3], eye))
    top = functools.reduce(jnp.maximum, lses)
    factors = [jnp.exp(lse - top) for lse in lses]
    total = functools.reduce(jnp.add, factors)
    acc = v_ref[...].astype(F32) * factors[0] + keep_ref[:rows] * factors[1]
    for ref, factor in zip(arrived, factors[2:]):
        acc = acc + ref[:rows].astype(F32) * factor
    hold_ref[...] = acc / total
    for j in range(per_dev):
        out_ref[:, j * HD : (j + 1) * HD] = hold_ref[pl.ds(j, seqs, stride=per_dev), :].astype(BF16)


def project_kernel(where_ref, x_ref, w_ref, o_ref):
    o_ref[0] = jnp.dot(x_ref[...], w_ref[...], preferred_element_type=F32)


def norm_kernel(chips, full, where_ref, gain_ref, *refs):
    pieces, out_ref = refs[: 2 * chips], refs[2 * chips]
    t, k = where_ref[0], where_ref[1]
    width = pieces[0].shape[1]
    total = jnp.zeros((pieces[0].shape[0], HD), F32)
    for ref in pieces:
        for c in range(0, width, HD):
            wide = ref[:, c : c + HD].astype(F32)
            total = total + wide * wide
    inverse = lax.rsqrt(jnp.sum(total, axis=1, keepdims=True) / full + epsilon)
    for index, ref in enumerate(pieces):
        side, s = index // chips, index % chips
        place = ((t - s + chips) % chips) * 2 + (k if side == 0 else 1 - k)
        at = pl.ds(pl.multiple_of(place * width, width), width)
        out_ref[:, at] = (ref[...].astype(F32) * inverse * gain_ref[:, at]).astype(BF16)


def on_device(chips, residual, query, new_pair, kv_cache, lengths, out_weight, norm_gain):
    seqs, width = residual.shape
    per_dev = query.shape[1] // HD
    span, kvh = kv_cache.shape[2], kv_cache.shape[3]
    heads = 2 * chips * per_dev
    group = heads // kvh
    rows = seqs * per_dev
    t, k = lax.axis_index("tensor"), lax.axis_index("kv")
    mine = t * 2 + k
    where = jnp.stack([t, k, mine * span]).astype(jnp.int32)

    def hop(x, s):
        return lax.ppermute(x, "tensor", [(i, (i + s) % chips) for i in range(chips)])

    def swap(x):
        return lax.ppermute(x, "kv", [(0, 1), (1, 0)])

    def everywhere(x):
        own = [x] + [hop(x, s) for s in range(1, chips)]
        return own + [swap(piece) for piece in own]

    vmem = pl.BlockSpec(memory_space=pltpu.VMEM)
    smem = pl.BlockSpec(memory_space=pltpu.SMEM)

    own_query = query.reshape(seqs, per_dev, HD)
    queries = jnp.concatenate(everywhere(own_query), axis=1)
    cache = kv_cache.reshape(2, seqs, span * kvh, HD)

    step_seqs = 4
    packed = jax.ShapeDtypeStruct((chips + 1, seqs, per_dev, HD), F32)
    whole_block = pl.BlockSpec((chips + 1, seqs, per_dev, HD), lambda i: (0, 0, 0, 0))
    own, par = pl.pallas_call(
        functools.partial(attention_kernel, chips, per_dev, kvh, group, step_seqs),
        grid=(seqs // step_seqs,),
        in_specs=[
            smem,
            smem,
            pl.BlockSpec((step_seqs, heads, HD), lambda i: (i, 0, 0)),
            pl.BlockSpec((2, step_seqs, span * kvh, HD), lambda i: (0, i, 0, 0)),
        ],
        out_specs=[whole_block, whole_block],
        out_shape=[packed, packed],
        scratch_shapes=[pltpu.VMEM((2, chips, seqs, per_dev, HD), F32)],
        compiler_params=pltpu.CompilerParams(
            dimension_semantics=("arbitrary",), vmem_limit_bytes=52 << 20
        ),
        cost_estimate=cost(4 * seqs * heads * span * kvh * HD, cache.size * 2),
        name="attention",
    )(where, lengths, queries, cache)

    sent = swap(par)
    merged = pl.pallas_call(
        functools.partial(pair_kernel, chips, per_dev),
        in_specs=[vmem, vmem],
        out_specs=[vmem] * chips,
        out_shape=[jax.ShapeDtypeStruct((rows + 8, HD), F32)]
        + [jax.ShapeDtypeStruct((rows + 16, HD), BF16)] * (chips - 1),
        compiler_params=pltpu.CompilerParams(vmem_limit_bytes=8 << 20),
        name="pair_merge",
    )(own, sent)
    arrived = [hop(merged[s], chips - s) for s in range(1, chips)]

    fresh_pair = lax.dynamic_index_in_dim(new_pair, mine * per_dev // group, 2, keepdims=False)
    fresh_pair = jnp.broadcast_to(fresh_pair[:, :, None, :], (2, seqs, per_dev, HD)).reshape(2, rows, HD)
    attended = pl.pallas_call(
        functools.partial(owner_kernel, chips, per_dev),
        in_specs=[vmem] * (chips + 3),
        out_specs=vmem,
        out_shape=jax.ShapeDtypeStruct((seqs, per_dev * HD), BF16),
        scratch_shapes=[pltpu.VMEM((rows, HD), F32)],
        compiler_params=pltpu.CompilerParams(vmem_limit_bytes=8 << 20),
        name="owner_merge",
    )(own_query.reshape(rows, HD), fresh_pair[0], fresh_pair[1], merged[0], *arrived)

    depth = out_weight.shape[0]
    tile = min(width, 1024)
    cut = width // tile

    def project(other):
        def column(s, c, at):
            side = 1 - at[1] if other else at[1]
            return (0, (((at[0] - s + chips) % chips) * 2 + side) * cut + c)

        return pl.pallas_call(
            project_kernel,
            grid_spec=pltpu.PrefetchScalarGridSpec(
                num_scalar_prefetch=1,
                grid=(chips, cut),
                in_specs=[
                    pl.BlockSpec((seqs, depth), lambda s, c, at: (0, 0)),
                    pl.BlockSpec((depth, tile), column),
                ],
                out_specs=pl.BlockSpec((1, seqs, tile), lambda s, c, at: (s, 0, c)),
            ),
            out_shape=jax.ShapeDtypeStruct((chips, seqs, width), F32),
            compiler_params=pltpu.CompilerParams(
                dimension_semantics=("arbitrary", "arbitrary"), vmem_limit_bytes=40 << 20
            ),
            cost_estimate=cost(
                2 * seqs * depth * width * chips, depth * width * chips * 2
            ),
            name="project_other" if other else "project_own",
        )(where, attended, out_weight)

    theirs = swap(project(True))
    ours = project(False)
    share = residual.astype(F32) + (ours[0] + theirs[0])
    for s in range(1, chips):
        share = share + hop((ours[s] + theirs[s]).astype(BF16), chips - s).astype(F32)
    stream = share.astype(BF16)

    pieces = everywhere(stream)
    normed = pl.pallas_call(
        functools.partial(norm_kernel, chips, width * chips * 2),
        in_specs=[smem] + [vmem] * (1 + 2 * chips),
        out_specs=vmem,
        out_shape=jax.ShapeDtypeStruct((seqs, width * chips * 2), BF16),
        compiler_params=pltpu.CompilerParams(vmem_limit_bytes=8 << 20),
        name="norm",
    )(where, norm_gain.astype(F32)[None, :], *pieces)
    return (stream, normed)


def solution(mesh):
    placed = (
        P(("groups", "dp"), ("tensor", "kv")),
        P(("groups", "dp"), ("tensor", "kv")),
        P(None, ("groups", "dp"), None, None),
        P(None, ("groups", "dp"), ("tensor", "kv"), None, None),
        P(("groups", "dp")),
        P(("tensor", "kv"), None),
        P(),
    )
    return jax.shard_map(
        functools.partial(on_device, mesh.shape["tensor"]),
        mesh=mesh,
        in_specs=placed,
        out_specs=(P(("groups", "dp"), ("tensor", "kv")), P(("groups", "dp"), None)),
        check_vma=False,
    )
```
